16 devices in a mesh: dp: 1, tp: 16 (over x, y, z, core).
Axes of the slice: x: 2, y: 2, z: 2, core: 2. Of those that a mesh axis runs over, the one named last changes fastest.
Arguments:
- x: bfloat16 [2048, 4096], P('dp')
- dy: bfloat16 [2048, 4096], P('dp')
- gate: bfloat16 [2048, 10240], P('dp', 'tp')
- up: bfloat16 [2048, 10240], P('dp', 'tp')
- w_gate: bfloat16 [4096, 10240], P(None, 'tp')
- w_up: bfloat16 [4096, 10240], P(None, 'tp')
- w_down: bfloat16 [10240, 4096], P('tp')
Outputs:
- output 1: bfloat16 [2048, 4096], P('dp')
- output 2: bfloat16 [4096, 10240], P('dp', 'tp')
- output 3: bfloat16 [4096, 10240], P('dp', 'tp')
- output 4: bfloat16 [10240, 4096], P(('dp', 'tp'))
All inputs are finite; a program needn't handle non-finite values.
Results may differ from the reference program's by a relative error of at most 0.012.
Values are sent between devices in bfloat16 or wider.
A program may use at most 2 GiB of HBM per device.

```python
import jax
import jax.numpy as jnp

ROWS = 2048
D = 4096
FF = 10240


def act(gate, up):
    return jax.nn.gelu(gate) * up


def setup_inputs(seed: int = 0, part: int = 0) -> dict:
    kx, ky, ka, kb, kg, ku, kd = jax.random.split(jax.random.key(seed), 7)
    kx, ky, ka, kb = (jax.random.fold_in(k, part) for k in (kx, ky, ka, kb))
    drawn = {
        "x": jax.random.normal(kx, (ROWS, D), jnp.float32),
        "dy": jax.random.normal(ky, (ROWS, D), jnp.float32),
        "gate": jax.random.normal(ka, (ROWS, FF), jnp.float32),
        "up": jax.random.normal(kb, (ROWS, FF), jnp.float32),
        "w_gate": jax.random.normal(kg, (D, FF), jnp.float32) * D**-0.5,
        "w_up": jax.random.normal(ku, (D, FF), jnp.float32) * D**-0.5,
        "w_down": jax.random.normal(kd, (FF, D), jnp.float32) * FF**-0.5,
    }
    return {k: v.astype(jnp.bfloat16) for k, v in drawn.items()}


def reference(x, dy, gate, up, w_gate, w_up, w_down):
    hidden, back = jax.vjp(act, gate.astype(jnp.float32), up.astype(jnp.float32))
    d_hidden = jnp.dot(dy, w_down.T, preferred_element_type=jnp.float32)
    d_gate, d_up = (g.astype(jnp.bfloat16) for g in back(d_hidden))
    dx = jnp.dot(d_gate, w_gate.T, preferred_element_type=jnp.float32) + jnp.dot(d_up, w_up.T, preferred_element_type=jnp.float32)
    dw_gate = jnp.dot(x.T, d_gate, preferred_element_type=jnp.float32)
    dw_up = jnp.dot(x.T, d_up, preferred_element_type=jnp.float32)
    dw_down = jnp.dot(hidden.astype(jnp.bfloat16).T, dy, preferred_element_type=jnp.float32)
    return tuple(g.astype(jnp.bfloat16) for g in (dx, dw_gate, dw_up, dw_down))
```

```python
import functools

import jax
import jax.numpy as jnp
from jax import lax
from jax.experimental import pallas as pl
from jax.experimental.pallas import tpu as pltpu
from jax.sharding import PartitionSpec as P

MESH = pl.DeviceIdType.MESH
BF16, F32 = jnp.bfloat16, jnp.float32

ROWS, D, F = 2048, 4096, 640
HALF = ROWS // 2
CW = 256
K = D // CW
BLOCK, SEG = 512, 128

PIECE = (32, 48, 48)
BASE = (0, 512, 1280)
OFF = tuple(tuple(n * o for o in (0, 32, 80)) for n in (8, 4, 2, 1))

LAG_B, LAG_C, LAG_D, LAG_E, LAG_F, LAG_G, LAG_H, LAG_I = 1, 3, 5, 7, 9, 11, 13, 15
STEPS = K + LAG_I
UNIT0 = 8
RING = 8
SENDS = 4


def act(gate, up):
    return jax.nn.gelu(gate) * up


def dot(a, b, ca, cb):
    return lax.dot_general(a, b, (((ca,), (cb,)), ((), ())), preferred_element_type=F32)


def source_row(half, seg):
    return jnp.where(
        seg < 2,
        256 * half + SEG * seg,
        jnp.where(seg < 5, 512 + 384 * half + SEG * (seg - 2), 1280 + 384 * half + SEG * (seg - 5)),
    )


def rows_at(start, n):
    return pl.ds(pl.multiple_of(start, 16), n)


def kernel(
    x, dy, gate, up, w_gate, w_up, w_down, dx, dw_gate, dw_up, dw_down,
    d, ht, w, own, ds, dr, s1, s2, s3, r1, r2, r3, fin,
    w_sem, ds_sem, dr_sem, s_sem, r_sem, fin_sem, as_sem, ar_sem, in_sem, out_sem,
):
    me = lax.axis_index("tp")
    core = me % 2
    bits = ((me // 8) % 2, (me // 4) % 2, (me // 2) % 2)
    step_of = (8, 4, 2)
    partner_core = me + 1 - 2 * core
    partners = tuple(me + s - 2 * s * b for s, b in zip(step_of, bits))

    barrier = pltpu.get_barrier_semaphore()
    for other in (partner_core, *partners):
        pl.semaphore_signal(barrier, inc=1, device_id={"tp": other}, device_id_type=MESH)
    pl.semaphore_wait(barrier, 4)

    def pick(axis, values):
        return jnp.where(axis == 0, values[0], jnp.where(axis == 1, values[1], values[2]))

    def remote(src, dst, send, recv, to):
        return pltpu.make_async_remote_copy(
            src_ref=src, dst_ref=dst, send_sem=send, recv_sem=recv, device_id={"tp": to}, device_id_type=MESH
        )

    def w_copies():
        return (
            pltpu.make_async_copy(w_gate, w.at[:, 0:F], w_sem.at[0]),
            pltpu.make_async_copy(w_up, w.at[:, F : 2 * F], w_sem.at[1]),
        )

    def first(wd, dyb, gb, ub, wd_sem, b_sem):
        def loads(b):
            slot = b % 2
            for s in range(BLOCK // SEG):
                src = pl.ds(pl.multiple_of(source_row(b // 2, (b % 2) * (BLOCK // SEG) + s), SEG), SEG)
                to = pl.ds(s * SEG, SEG)
                yield pltpu.make_async_copy(dy.at[src, :], dyb.at[slot, to, :], b_sem.at[slot, s, 0])
                yield pltpu.make_async_copy(gate.at[src, :], gb.at[slot, to, :], b_sem.at[slot, s, 1])
                yield pltpu.make_async_copy(up.at[src, :], ub.at[slot, to, :], b_sem.at[slot, s, 2])

        wd_copy = pltpu.make_async_copy(w_down, wd, wd_sem)
        wd_copy.start()
        for c in loads(0):
            c.start()

        def body(b, _):
            @pl.when(b + 1 < ROWS // BLOCK)
            def _():
                for c in loads(b + 1):
                    c.start()

            @pl.when(b == 0)
            def _():
                wd_copy.wait()
                for c in w_copies():
                    c.start()

            for c in loads(b):
                c.wait()
            slot = b % 2
            rows = pl.ds(pl.multiple_of(b * BLOCK, BLOCK), BLOCK)
            for lo, hi in ((0, 256), (256, 512), (512, F)):
                d_hidden = dot(dyb[slot], wd[lo:hi, :], 1, 1)
                hidden, back = jax.vjp(act, gb[slot, :, lo:hi].astype(F32), ub[slot, :, lo:hi].astype(F32))
                d_gate, d_up = back(d_hidden)
                d[rows, lo:hi] = d_gate.astype(BF16)
                d[rows, F + lo : F + hi] = d_up.astype(BF16)
                ht[lo:hi, rows] = hidden.T.astype(BF16)
            return 0

        lax.fori_loop(0, ROWS // BLOCK, body, 0)
        for c in w_copies():
            c.wait()

    pl.run_scoped(
        first,
        pltpu.VMEM((F, D), BF16),
        pltpu.VMEM((2, BLOCK, D), BF16),
        pltpu.VMEM((2, BLOCK, F), BF16),
        pltpu.VMEM((2, BLOCK, F), BF16),
        pltpu.SemaphoreType.DMA,
        pltpu.SemaphoreType.DMA((2, BLOCK // SEG, 3)),
    )

    def second(xb, yb, ob, oc):
        def tile_loads(u):
            slot = u % 2
            cols = pl.ds(pl.multiple_of(u * CW, CW), CW)
            for half in range(2):
                for g in range(3):
                    n = 8 * PIECE[g]
                    src = pl.ds(BASE[g] + half * n, n)
                    to = pl.ds(half * HALF + OFF[0][g], n)
                    yield pltpu.make_async_copy(x.at[src, cols], xb.at[slot, to, :], in_sem.at[slot, 0, half, g])
                    yield pltpu.make_async_copy(dy.at[src, cols], yb.at[slot, to, :], in_sem.at[slot, 1, half, g])

        def tile_stores(u):
            slot = u % 2
            at = pl.ds(pl.multiple_of(u * CW, CW), CW)
            yield pltpu.make_async_copy(ob.at[slot, :, 0:F], dw_gate.at[at, :], out_sem.at[slot, 0])
            yield pltpu.make_async_copy(ob.at[slot, :, F : 2 * F], dw_up.at[at, :], out_sem.at[slot, 1])
            yield pltpu.make_async_copy(oc.at[slot], dw_down.at[:, at], out_sem.at[slot, 2])

        def d2d(j):
            return remote(ds.at[j % 2], dr.at[j % SENDS], ds_sem.at[j % 2], dr_sem.at[j % SENDS], partner_core)

        sent, got = (s1, s2, s3), (r1, r2, r3)

        def scatter(stage, g, j):
            n = PIECE[g] * (4, 2, 1)[stage]
            at = pl.ds(OFF[stage + 1][g], n)
            return remote(
                sent[stage].at[j % SENDS, at, :],
                got[stage].at[j, at, :],
                s_sem.at[stage, g, j % SENDS],
                r_sem.at[stage, g, j],
                pick((g + j + stage) % 3, partners),
            )

        def place(g, j, stage, theirs):
            p = PIECE[g]
            ba, bb, bc = (pick((g + j + s) % 3, bits) for s in range(3))
            if stage == 0:
                at = 8 * core + 4 * ba + 2 * bb + (1 - bc if theirs else bc)
            elif stage == 1:
                at = 8 * core + 4 * ba + 2 * (1 - bb if theirs else bb)
            elif stage == 2:
                at = 8 * core + 4 * (1 - ba if theirs else ba)
            else:
                at = 8 * (1 - core if theirs else core)
            n = p * (1, 2, 4, 8)[stage]
            return dx.at[rows_at(BASE[g] + p * at, n), pl.ds(pl.multiple_of(j * CW, CW), CW)]

        def fin_at(g, j):
            return fin.at[j % SENDS, pl.ds(OFF[3][g], PIECE[g]), :]

        def fin_copy(g, j):
            return pltpu.make_async_copy(fin_at(g, j), place(g, j, 0, False), fin_sem.at[g, j % SENDS])

        def gather(stage, g, j, theirs):
            spot = place(g, j, stage, theirs)
            to = partner_core if stage == 3 else pick((g + j + 2 - stage) % 3, partners)
            src = fin_at(g, j) if stage == 0 else spot
            return remote(src, spot, as_sem.at[stage, g, j % SENDS], ar_sem.at[stage, g, j], to)

        def when_chunk(i, lag):
            j = i - lag
            return j, pl.when(jnp.logical_and(j >= 0, j < K))

        def body(i, _):
            @pl.when(i < K)
            def _():
                wt = pl.ds(pl.multiple_of(i * CW, CW), CW)

                @pl.when(i >= 2)
                def _():
                    d2d(i - 2).wait_send()

                def part(half, r):
                    rows = pl.ds(pl.multiple_of(half * HALF + r * BLOCK, BLOCK), BLOCK)
                    return dot(d[rows, :], w[wt, :], 1, 1), pl.ds(pl.multiple_of(r * BLOCK, BLOCK), BLOCK)

                @pl.loop(0, HALF // BLOCK)
                def _(r):
                    term, at = part(1 - core, r)
                    ds[i % 2, at, :] = term.astype(BF16)

                d2d(i).start()

                @pl.loop(0, HALF // BLOCK)
                def _(r):
                    term, at = part(core, r)
                    own[i % RING, at, :] = term

            j, valid = when_chunk(i, LAG_B)

            @valid
            def _():
                d2d(j).wait_recv()
                for g in range(3):
                    n = 4 * PIECE[g]
                    bit = pick((g + j) % 3, bits)
                    keep = rows_at(OFF[0][g] + n * bit, n)
                    give = rows_at(OFF[0][g] + n * (1 - bit), n)
                    at = pl.ds(OFF[1][g], n)

                    @pl.when(j >= SENDS)
                    def _():
                        scatter(0, g, j - SENDS).wait_send()

                    s1[j % SENDS, at, :] = (own[j % RING, give, :] + dr[j % SENDS, give, :].astype(F32)).astype(BF16)
                    scatter(0, g, j).start()
                    own[j % RING, keep, :] = own[j % RING, keep, :] + dr[j % SENDS, keep, :].astype(F32)

            for stage, lag in ((1, LAG_C), (2, LAG_D)):
                j, valid = when_chunk(i, lag)

                @valid
                def _(j=j, stage=stage):
                    for g in range(3):
                        scatter(stage - 1, g, j).wait_recv()
                        n = PIECE[g] * (4, 2, 1)[stage]
                        bs = [pick((g + j + s) % 3, bits) for s in range(stage + 1)]
                        start = OFF[0][g] + sum(PIECE[g] * (4, 2, 1)[s] * bs[s] for s in range(stage))
                        bit = bs[stage]
                        keep, give = rows_at(start + n * bit, n), rows_at(start + n * (1 - bit), n)
                        base = OFF[stage][g]
                        rkeep, rgive = rows_at(base + n * bit, n), rows_at(base + n * (1 - bit), n)
                        at = pl.ds(OFF[stage + 1][g], n)

                        @pl.when(j >= SENDS)
                        def _():
                            scatter(stage, g, j - SENDS).wait_send()

                        r = got[stage - 1]
                        sent[stage][j % SENDS, at, :] = (
                            own[j % RING, give, :] + r[j, rgive, :].astype(F32)
                        ).astype(BF16)
                        scatter(stage, g, j).start()
                        own[j % RING, keep, :] = own[j % RING, keep, :] + r[j, rkeep, :].astype(F32)

            j, valid = when_chunk(i, LAG_E)

            @valid
            def _():
                for g in range(3):
                    scatter(2, g, j).wait_recv()
                    n = PIECE[g]
                    bs = [pick((g + j + s) % 3, bits) for s in range(3)]
                    keep = rows_at(OFF[0][g] + sum(n * (4, 2, 1)[s] * bs[s] for s in range(3)), n)
                    at = pl.ds(OFF[3][g], n)

                    @pl.when(j >= SENDS)
                    def _():
                        gather(0, g, j - SENDS, False).wait_send()

                    fin[j % SENDS, at, :] = (own[j % RING, keep, :] + r3[j, at, :].astype(F32)).astype(BF16)
                    fin_copy(g, j).start()
                    gather(0, g, j, False).start()

            for stage, lag in ((1, LAG_F), (2, LAG_G), (3, LAG_H)):
                j, valid = when_chunk(i, lag)

                @valid
                def _(j=j, stage=stage):
                    for g in range(3):
                        gather(stage - 1, g, j, True).wait_recv()
                        if stage == 1:
                            fin_copy(g, j).wait()

                        @pl.when(j >= SENDS)
                        def _():
                            gather(stage, g, j - SENDS, False).wait_send()

                        gather(stage, g, j, False).start()

            j, valid = when_chunk(i, LAG_I)

            @valid
            def _():
                for g in range(3):
                    gather(3, g, j, True).wait_recv()

            u = i - UNIT0

            @pl.when(u == -1)
            def _():
                for c in tile_loads(0):
                    c.start()

            @pl.when(jnp.logical_and(u >= 0, u < K))
            def _():
                @pl.when(u + 1 < K)
                def _():
                    for c in tile_loads(u + 1):
                        c.start()

                for c in tile_loads(u):
                    c.wait()

                @pl.when(u >= 2)
                def _():
                    for c in tile_stores(u - 2):
                        c.wait()

                slot = u % 2
                ob[slot] = dot(xb[slot], d[...], 0, 0).astype(BF16)
                oc[slot] = dot(ht[...], yb[slot], 1, 0).astype(BF16)
                for c in tile_stores(u):
                    c.start()

            return 0

        lax.fori_loop(0, STEPS, body, 0)

        for u in (K - 2, K - 1):
            for c in tile_stores(u):
                c.wait()
        for j in (K - 2, K - 1):
            d2d(j).wait_send()
        for j in range(K - SENDS, K):
            for g in range(3):
                for stage in range(3):
                    scatter(stage, g, j).wait_send()
                for stage in range(4):
                    gather(stage, g, j, False).wait_send()

    pl.run_scoped(
        second,
        pltpu.VMEM((2, ROWS, CW), BF16),
        pltpu.VMEM((2, ROWS, CW), BF16),
        pltpu.VMEM((2, CW, 2 * F), BF16),
        pltpu.VMEM((2, F, CW), BF16),
    )


def solution(mesh):
    def step(x, dy, gate, up, w_gate, w_up, w_down):
        shape = lambda *s: jax.ShapeDtypeStruct(s, BF16)
        anywhere = pl.BlockSpec(memory_space=pl.ANY)
        dma = pltpu.SemaphoreType.DMA
        return pl.pallas_call(
            kernel,
            out_shape=(shape(ROWS, D), shape(D, F), shape(D, F), shape(F, D)),
            in_specs=[anywhere] * 7,
            out_specs=(anywhere,) * 4,
            scratch_shapes=[
                pltpu.VMEM((ROWS, 2 * F), BF16),
                pltpu.VMEM((F, ROWS), BF16),
                pltpu.VMEM((D, 2 * F), BF16),
                pltpu.VMEM((RING, HALF, CW), F32),
                pltpu.VMEM((2, HALF, CW), BF16),
                pltpu.VMEM((SENDS, HALF, CW), BF16),
                pltpu.VMEM((SENDS, 512, CW), BF16),
                pltpu.VMEM((SENDS, 256, CW), BF16),
                pltpu.VMEM((SENDS, 128, CW), BF16),
                pltpu.VMEM((K, 512, CW), BF16),
                pltpu.VMEM((K, 256, CW), BF16),
                pltpu.VMEM((K, 128, CW), BF16),
                pltpu.VMEM((SENDS, 128, CW), BF16),
                dma((2,)),
                dma((2,)),
                dma((SENDS,)),
                dma((3, 3, SENDS)),
                dma((3, 3, K)),
                dma((3, SENDS)),
                dma((4, 3, SENDS)),
                dma((4, 3, K)),
                dma((2, 2, 2, 3)),
                dma((2, 3)),
            ],
            compiler_params=pltpu.CompilerParams(
                collective_id=0, has_side_effects=True, vmem_limit_bytes=67043328
            ),
        )(x, dy, gate, up, w_gate, w_up, w_down)

    tokens, columns, rows = P("dp", None), P(None, "tp"), P("tp", None)
    return jax.shard_map(
        step,
        mesh=mesh,
        in_specs=(tokens, tokens, P("dp", "tp"), P("dp", "tp"), columns, columns, rows),
        out_specs=(tokens, P("dp", "tp"), P("dp", "tp"), P(("dp", "tp"), None)),
        check_vma=False,
    )
```
